32 devices in a mesh: band: 8 (over y, x, core), grid: 4 (over z).
Axes of the slice: x: 2, y: 2, z: 4, core: 2. Of those that a mesh axis runs over, the one named last changes fastest.
Arguments:
- wave: bfloat16 [4096, 10240], P('band', 'grid'), may hold values from -6 to 6
- ritz: bfloat16 [4096, 4096], P('band', 'grid'), may hold values from -0.125 to 0.125
- occupation: float32 [4096], P('band'), may hold values from 0 to 2
Outputs:
- rotated: bfloat16 [4096, 10240], P('band', 'grid')
- density: float32 [10240], P('grid')
The draws below stay inside these ranges and needn't reach their ends.
All inputs are finite; a program needn't handle non-finite values.
Results may differ from the reference program's by a relative error of at most 0.0017.
Values may be sent and summed in bfloat16 or wider, within the bound.
A program may use at most 128 MiB of HBM per device.

```python
import jax
import jax.numpy as jnp
from jax import lax

NB = 4096
CELLS = 10240


def strengthened(values, stream_key, source, target, blocks, factor):
    def block_of(position):
        return (jnp.arange(values.shape[position]) // (values.shape[position] // blocks)).reshape((-1,) + (1,) * (values.ndim - 1 - position))

    first = jax.random.permutation(stream_key, blocks)[block_of(target)]
    other_side = (block_of(target) + blocks // 2) % blocks
    return jnp.where((block_of(source) == first) | (block_of(source) == other_side), factor * values, values)


def shard_levels(rng, extent, pieces, low, high):
    factor_of = 1.0
    for axis_at, blocks in pieces:
        heights = jax.random.uniform(jax.random.fold_in(jax.random.fold_in(rng, 6), axis_at), (blocks,), jnp.float32, low / len(pieces), high / len(pieces))
        factor_of = factor_of * jnp.repeat(jnp.exp(heights), extent[axis_at] // blocks).reshape((-1,) + (1,) * (len(extent) - 1 - axis_at))
    return factor_of


def bell_draw(rng, extent, deviation, most, cuts=(), held_as=jnp.bfloat16):
    array = jax.random.normal(rng, extent, jnp.float32) * deviation
    if len(cuts) > 0:
        array = shard_levels(rng, extent, cuts, -0.22, 0.18) * array
    return jnp.clip(array, min=-most, max=most).astype(held_as)


def gaussian_with(rng, shape, spread, reach, shards, heavy, held_as=jnp.bfloat16):
    entries = spread * jax.random.normal(rng, shape, jnp.float32)
    if shards:
        entries = entries * shard_levels(rng, shape, shards, -0.22, 0.18)
    return jnp.clip(strengthened(entries, jax.random.fold_in(rng, 3), *heavy), -reach, reach).astype(held_as)


def setup_inputs(seed: int = 0) -> dict:
    keys = jax.random.split(jax.random.key(seed), 4)
    return {
        "wave": bell_draw(keys[0], (NB, CELLS), 1.0, 6.0, ((0, 8), (1, 4))),
        "ritz": gaussian_with(keys[1], (NB, NB), NB ** -0.5, 0.125, ((0, 8), (1, 4)), (0, 1, 8, 2.0)),
        "occupation": jnp.clip(2.0 * jax.random.uniform(keys[2], (NB,), jnp.float32) ** shard_levels(keys[2], (NB,), ((0, 8),), -0.2, 0.2), 0.0, 2.0),
    }


def reference(wave, ritz, occupation):
    summed = jnp.dot(ritz.astype(jnp.float32).T, wave.astype(jnp.float32), precision=lax.Precision.HIGHEST)
    rotated = summed.astype(jnp.bfloat16)
    values = rotated.astype(jnp.float32)
    density = jnp.sum(occupation[:, None] * values * values, axis=0) / NB
    return rotated, density
```

```python
import functools

import jax
import jax.numpy as jnp
from jax import lax
from jax.experimental import pallas as pl
from jax.experimental.pallas import tpu as pltpu
from jax.sharding import PartitionSpec as P

MESH = pl.DeviceIdType.MESH
CHUNKS = 4


def chip_at(p, chips):
    p = lax.rem(p + chips, chips)
    back = (2 * p) // chips
    return (1 - back) * (2 * p) + back * (2 * (chips - 1 - p) + 1)


def kernel(
    nb, ng, wave, ritz, occ, rotated, density,
    w_all, z_all, a_buf, z_t, total, out_buf, d_all,
    a_send, a_recv, b_send, b_recv, up_send, dn_send, z_recv,
    r_send, l_send, d_send, w_recv, q_send, q_recv, o_sem,
):
    chips = nb // 2
    half = chips // 2
    rows, cells = wave.shape
    cols = z_all.shape[1]
    quarter = rows // ng
    crows = rows // CHUNKS
    me = lax.axis_index("band")
    g = lax.axis_index("grid")
    core = lax.rem(me, 2)
    chip = me // 2
    odd = lax.rem(chip, 2)
    place = (1 - odd) * (chip // 2) + odd * (chips - 1 - chip // 2)
    partner = me + 1 - 2 * core

    barrier = pltpu.get_barrier_semaphore()
    for d in range(1, nb):
        pl.semaphore_signal(barrier, inc=1, device_id={"band": lax.rem(me + d, nb), "grid": g}, device_id_type=MESH)
    for d in range(1, ng):
        pl.semaphore_signal(barrier, inc=1, device_id={"band": me, "grid": lax.rem(g + d, ng)}, device_id_type=MESH)
    pl.semaphore_wait(barrier, nb - 1 + ng - 1)

    def remote(src, dst, send, recv, band, grid):
        return pltpu.make_async_remote_copy(
            src_ref=src, dst_ref=dst, send_sem=send, recv_sem=recv,
            device_id={"band": band, "grid": grid}, device_id_type=MESH,
        )

    def a_copy(to):
        return remote(
            ritz.at[pl.ds(pl.multiple_of(to * quarter, quarter), quarter), :],
            a_buf.at[g], a_send.at[to], a_recv.at[g], me, to,
        )

    for d in range(1, ng):
        a_copy(lax.rem(g + d, ng)).start()
    a_own = pltpu.make_async_copy(
        ritz.at[pl.ds(pl.multiple_of(g * quarter, quarter), quarter), :], a_buf.at[g], a_recv.at[g]
    )
    a_own.start()

    def slot(band, ch):
        return w_all.at[pl.ds(pl.multiple_of(band * rows + ch * crows, crows), crows), :]

    def own_chunk(ch):
        return wave.at[pl.ds(ch * crows, crows), :]

    def ring_copy(step, d, ch):
        band = chip_at(place - step * d, chips) * 2 + core
        to = chip_at(place + step, chips) * 2 + core
        sems = r_send if step > 0 else l_send
        src = own_chunk(ch) if d == 0 else slot(band, ch)
        return remote(src, slot(band, ch), sems.at[d, ch], w_recv.at[band, ch], to, g)

    def pair_copy(band, ch, first):
        src = own_chunk(ch) if first else slot(band, ch)
        return remote(src, slot(band, ch), d_send.at[band // 2, ch], w_recv.at[band, ch], partner, g)

    low = list(range(CHUNKS // 2))
    high = list(range(CHUNKS // 2, CHUNKS))
    for a, b in zip(low, high):
        ring_copy(1, 0, a).start()
        ring_copy(-1, 0, b).start()
    for ch in range(CHUNKS):
        pltpu.make_async_copy(own_chunk(ch), slot(me, ch), w_recv.at[me, ch]).start()
        pair_copy(me, ch, True).start()

    def piece(band, q):
        return z_all.at[pl.ds(pl.multiple_of(band * rows + q * quarter, quarter), quarter), :]

    def b_copy(c, k):
        return remote(
            a_buf.at[c, :, pl.ds(k * cols, cols)], piece(me, g),
            b_send.at[2 * c + k], b_recv.at[me], 2 * c + k, g,
        )

    def b_local(c, k):
        return pltpu.make_async_copy(a_buf.at[c, :, pl.ds(k * cols, cols)], piece(me, g), b_recv.at[me])

    for d in range(ng):
        c = lax.rem(g + d, ng)
        remote(a_buf.at[c], a_buf.at[c], a_send.at[c], a_recv.at[c], me, g).wait_recv()
        for k in range(2):
            @pl.when(2 * c + k == me)
            def _():
                b_local(c, k).start()

            @pl.when(2 * c + k != me)
            def _():
                b_copy(c, k).start()

    for a, b in zip(high, low):
        ring_copy(1, 0, a).start()
        ring_copy(-1, 0, b).start()

    def z_copy(step, q, j):
        sems = up_send if step > 0 else dn_send
        return remote(piece(j, q), piece(j, q), sems.at[q, j], z_recv.at[q, j], me, g + step)

    def z_own(t, carry):
        j = lax.rem(me + t, nb)
        remote(piece(j, g), piece(j, g), b_send.at[j], b_recv.at[j], me, g).wait_recv()

        @pl.when(g < ng - 1)
        def _():
            z_copy(1, g, j).start()

        @pl.when(g > 0)
        def _():
            z_copy(-1, g, j).start()

        return carry

    lax.fori_loop(0, nb, z_own, 0)

    def z_step(t, carry):
        d = t // nb + 1
        j = lax.rem(me + t, nb)

        @pl.when(g - d >= 0)
        def _():
            z_copy(1, g - d, j).wait_recv()

            @pl.when(g < ng - 1)
            def _():
                z_copy(1, g - d, j).start()

        @pl.when(g + d < ng)
        def _():
            z_copy(-1, g + d, j).wait_recv()

            @pl.when(g > 0)
            def _():
                z_copy(-1, g + d, j).start()

        return carry

    events = []
    for d in range(1, half):
        events += [(d, a, b) for a, b in zip(low + high, high + low)]
    events += [(half, a, b) for a, b in zip(low, high)]

    def arrive(step, d, ch):
        band = chip_at(place - step * d, chips) * 2 + core
        ring_copy(step, d, ch).wait_recv()
        pair_copy(band, ch, False).start()
        mine = low if step > 0 else high
        if d + 1 < half or (d + 1 == half and ch in mine):
            ring_copy(step, d, ch).start()

    def wait_pair(band, ch):
        pair_copy(band, ch, False).wait_recv()

    tile = max(t for t in range(128, 513, 128) if cells % t == 0)
    depth = 2 * rows

    def load_t(c):
        z_t[...] = z_all[pl.ds(pl.multiple_of(c * depth, depth), depth), :].T

    def product(c, at):
        return jnp.dot(
            z_t[...], w_all[pl.ds(pl.multiple_of(c * depth, depth), depth), at],
            preferred_element_type=jnp.float32,
        )

    def add_chip(c, first):
        load_t(c)

        @pl.loop(0, cells // tile)
        def _(i):
            at = pl.ds(pl.multiple_of(i * tile, tile), tile)
            if first:
                total[:, at] = product(c, at)
            else:
                total[:, at] += product(c, at)

    steps = (ng - 1) * nb
    spread = len(events) - 1
    for e, (d, a, b) in enumerate(events):
        if e == spread:
            for ch in range(CHUNKS):
                remote(slot(me, ch), slot(me, ch), d_send.at[chip, ch], w_recv.at[me, ch], me, g).wait_recv()
                wait_pair(partner, ch)
            add_chip(chip, True)
            for dd in range(1, half):
                for step in (1, -1):
                    c = chip_at(place - step * dd, chips)
                    for ch in range(CHUNKS):
                        wait_pair(2 * c + 1 - core, ch)
                    add_chip(c, False)
        else:
            lax.fori_loop(steps * e // spread, steps * (e + 1) // spread, z_step, 0)
        arrive(1, d, a)
        arrive(-1, d, b)

    last = chip_at(place + half, chips)
    load_t(last)
    for ch in range(CHUNKS):
        wait_pair(2 * last + 1 - core, ch)

    @pl.loop(0, cells // tile)
    def _(i):
        at = pl.ds(pl.multiple_of(i * tile, tile), tile)
        rounded = (total[:, at] + product(last, at)).astype(jnp.bfloat16)
        out_buf[:, at] = rounded
        values = rounded.astype(jnp.float32)
        d_all[me, :, at] = jnp.sum(occ[...] * values * values, axis=0, keepdims=True)
        pltpu.make_async_copy(out_buf.at[:, at], rotated.at[:, at], o_sem.at[i]).start()

    def q_copy(to):
        return remote(d_all.at[me], d_all.at[me], q_send.at[to], q_recv.at[me], to, g)

    for d in range(1, nb):
        q_copy(lax.rem(me + d, nb)).start()

    for d in range(1, ng):
        a_copy(lax.rem(g + d, ng)).wait_send()

    def b_sent(to, carry):
        @pl.when(to != me)
        def _():
            remote(
                a_buf.at[0, :, pl.ds(0, cols)], piece(me, g), b_send.at[to], b_recv.at[me], to, g
            ).wait_send()

        return carry

    lax.fori_loop(0, nb, b_sent, 0)

    def z_sent(t, carry):
        q, j = t // nb, lax.rem(t, nb)

        @pl.when((q <= g) & (g < ng - 1))
        def _():
            z_copy(1, q, j).wait_send()

        @pl.when((q >= g) & (g > 0))
        def _():
            z_copy(-1, q, j).wait_send()

        return carry

    lax.fori_loop(0, ng * nb, z_sent, 0)
    for step in (1, -1):
        mine = low if step > 0 else high
        for d in range(half):
            for ch in (range(CHUNKS) if d + 1 < half else mine):
                ring_copy(step, d, ch).wait_send()
    for c in range(chips):
        for ch in range(CHUNKS):
            remote(slot(2 * c + core, ch), slot(2 * c + core, ch), d_send.at[c, ch], w_recv.at[2 * c + core, ch], partner, g).wait_send()

    for d in range(1, nb):
        src = lax.rem(me + d, nb)
        remote(d_all.at[src], d_all.at[src], q_send.at[src], q_recv.at[src], me, g).wait_recv()
    density[...] = jnp.sum(d_all[...], axis=0) / (nb * rows)
    for d in range(1, nb):
        q_copy(lax.rem(me + d, nb)).wait_send()

    @pl.loop(0, cells // tile)
    def _(i):
        at = pl.ds(pl.multiple_of(i * tile, tile), tile)
        pltpu.make_async_copy(out_buf.at[:, at], rotated.at[:, at], o_sem.at[i]).wait()


def solution(mesh):
    nb, ng = mesh.shape["band"], mesh.shape["grid"]

    def per_device(wave, ritz, occupation):
        rows, cells = wave.shape
        bands = rows * nb
        wide = ritz.shape[1]
        cols = bands // nb
        chips = nb // 2
        half = chips // 2
        dma = pltpu.SemaphoreType.DMA
        rotated, density = pl.pallas_call(
            functools.partial(kernel, nb, ng),
            out_shape=(
                jax.ShapeDtypeStruct((cols, cells), jnp.bfloat16),
                jax.ShapeDtypeStruct((1, cells), jnp.float32),
            ),
            in_specs=[
                pl.BlockSpec(memory_space=pl.ANY),
                pl.BlockSpec(memory_space=pl.ANY),
                pl.BlockSpec(memory_space=pltpu.VMEM),
            ],
            out_specs=(pl.BlockSpec(memory_space=pl.ANY), pl.BlockSpec(memory_space=pltpu.VMEM)),
            scratch_shapes=[
                pltpu.VMEM((bands, cells), jnp.bfloat16),
                pltpu.VMEM((bands, cols), jnp.bfloat16),
                pltpu.VMEM((ng, rows // ng, wide), jnp.bfloat16),
                pltpu.VMEM((cols, 2 * rows), jnp.bfloat16),
                pltpu.VMEM((cols, cells), jnp.float32),
                pltpu.VMEM((cols, cells), jnp.bfloat16),
                pltpu.VMEM((nb, 1, cells), jnp.float32),
                dma((ng,)), dma((ng,)), dma((nb,)), dma((nb,)),
                dma((ng, nb)), dma((ng, nb)), dma((ng, nb)),
                dma((half, CHUNKS)), dma((half, CHUNKS)), dma((chips, CHUNKS)), dma((nb, CHUNKS)),
                dma((nb,)), dma((nb,)), dma((cells // 128,)),
            ],
            compiler_params=pltpu.CompilerParams(
                collective_id=0, has_side_effects=True, vmem_limit_bytes=60 * 1024 * 1024
            ),
        )(wave, ritz, occupation[:, None])
        return rotated, density.reshape(cells)

    return jax.shard_map(
        per_device,
        mesh=mesh,
        in_specs=(P("band", "grid"), P("band", "grid"), P("band")),
        out_specs=(P("band", "grid"), P("grid")),
        check_vma=False,
    )
```

```python
import functools

import jax
import jax.numpy as jnp
from jax import lax
from jax.experimental import pallas as pl
from jax.experimental.pallas import tpu as pltpu
from jax.sharding import PartitionSpec as P

MESH = pl.DeviceIdType.MESH
CHUNKS = 8


def chip_at(p, chips):
    p = lax.rem(p + chips, chips)
    back = (2 * p) // chips
    return (1 - back) * (2 * p) + back * (2 * (chips - 1 - p) + 1)


def kernel(
    nb, ng, wave, ritz, occ, rotated, density,
    w_all, z_all, a_buf, z_t, total, out_buf, d_all, o_col,
    a_send, a_recv, b_send, b_recv, up_send, dn_send, z_recv,
    r_send, l_send, d_send, w_recv, q_send, q_recv, o_sem,
):
    chips = nb // 2
    half = chips // 2
    rows, cells = wave.shape
    cols = z_all.shape[1]
    quarter = rows // ng
    crows = rows // CHUNKS
    me = lax.axis_index("band")
    g = lax.axis_index("grid")
    core = lax.rem(me, 2)
    chip = me // 2
    odd = lax.rem(chip, 2)
    place = (1 - odd) * (chip // 2) + odd * (chips - 1 - chip // 2)
    partner = me + 1 - 2 * core

    barrier = pltpu.get_barrier_semaphore()
    for d in range(1, nb):
        pl.semaphore_signal(barrier, inc=1, device_id={"band": lax.rem(me + d, nb), "grid": g}, device_id_type=MESH)
    for d in range(1, ng):
        pl.semaphore_signal(barrier, inc=1, device_id={"band": me, "grid": lax.rem(g + d, ng)}, device_id_type=MESH)
    pl.semaphore_wait(barrier, nb - 1 + ng - 1)

    def remote(src, dst, send, recv, band, grid):
        return pltpu.make_async_remote_copy(
            src_ref=src, dst_ref=dst, send_sem=send, recv_sem=recv,
            device_id={"band": band, "grid": grid}, device_id_type=MESH,
        )

    def a_copy(to):
        return remote(
            ritz.at[pl.ds(pl.multiple_of(to * quarter, quarter), quarter), :],
            a_buf.at[g], a_send.at[to], a_recv.at[g], me, to,
        )

    for d in range(1, ng):
        a_copy(lax.rem(g + d, ng)).start()
    a_own = pltpu.make_async_copy(
        ritz.at[pl.ds(pl.multiple_of(g * quarter, quarter), quarter), :], a_buf.at[g], a_recv.at[g]
    )
    a_own.start()

    def slot(band, ch):
        return w_all.at[pl.ds(pl.multiple_of(band * rows + ch * crows, crows), crows), :]

    def own_chunk(ch):
        return wave.at[pl.ds(ch * crows, crows), :]

    def ring_copy(step, d, ch):
        band = chip_at(place - step * d, chips) * 2 + core
        to = chip_at(place + step, chips) * 2 + core
        sems = r_send if step > 0 else l_send
        src = own_chunk(ch) if d == 0 else slot(band, ch)
        return remote(src, slot(band, ch), sems.at[d, ch], w_recv.at[band, ch], to, g)

    def pair_copy(band, ch, first):
        src = own_chunk(ch) if first else slot(band, ch)
        return remote(src, slot(band, ch), d_send.at[band // 2, ch], w_recv.at[band, ch], partner, g)

    low = list(range(CHUNKS // 2))
    high = list(range(CHUNKS // 2, CHUNKS))
    waiting = list(zip(low + high, high + low))

    def send_own(count):
        for _ in range(min(count, len(waiting))):
            a, b = waiting.pop(0)
            ring_copy(1, 0, a).start()
            ring_copy(-1, 0, b).start()

    send_own(1)
    for ch in range(CHUNKS):
        pltpu.make_async_copy(own_chunk(ch), slot(me, ch), w_recv.at[me, ch]).start()
        pair_copy(me, ch, True).start()

    def piece(band, q):
        return z_all.at[pl.ds(pl.multiple_of(band * rows + q * quarter, quarter), quarter), :]

    def b_copy(c, k):
        return remote(
            a_buf.at[c, :, pl.ds(k * cols, cols)], piece(me, g),
            b_send.at[2 * c + k], b_recv.at[me], 2 * c + k, g,
        )

    def b_local(c, k):
        return pltpu.make_async_copy(a_buf.at[c, :, pl.ds(k * cols, cols)], piece(me, g), b_recv.at[me])

    for d in range(ng):
        c = lax.rem(g + d, ng)
        remote(a_buf.at[c], a_buf.at[c], a_send.at[c], a_recv.at[c], me, g).wait_recv()
        for k in range(2):
            @pl.when(2 * c + k == me)
            def _():
                b_local(c, k).start()

            @pl.when(2 * c + k != me)
            def _():
                b_copy(c, k).start()

        send_own(1)
    send_own(CHUNKS)
    o_col[...] = jnp.broadcast_to(occ[...], (128, cols)).T

    def z_copy(step, q, j):
        sems = up_send if step > 0 else dn_send
        return remote(piece(j, q), piece(j, q), sems.at[q, j], z_recv.at[q, j], me, g + step)

    def z_own(t, carry):
        j = lax.rem(me + t, nb)
        remote(piece(j, g), piece(j, g), b_send.at[j], b_recv.at[j], me, g).wait_recv()

        @pl.when(g < ng - 1)
        def _():
            z_copy(1, g, j).start()

        @pl.when(g > 0)
        def _():
            z_copy(-1, g, j).start()

        return carry

    lax.fori_loop(0, nb, z_own, 0)

    def z_step(t, carry):
        d = t // nb + 1
        j = lax.rem(me + t, nb)

        @pl.when(g - d >= 0)
        def _():
            z_copy(1, g - d, j).wait_recv()

            @pl.when(g < ng - 1)
            def _():
                z_copy(1, g - d, j).start()

        @pl.when(g + d < ng)
        def _():
            z_copy(-1, g + d, j).wait_recv()

            @pl.when(g > 0)
            def _():
                z_copy(-1, g + d, j).start()

        return carry

    events = []
    for d in range(1, half):
        events += [(d, a, b) for a, b in zip(low + high, high + low)]
    events += [(half, a, b) for a, b in zip(low, high)]

    def arrive(step, d, ch):
        band = chip_at(place - step * d, chips) * 2 + core
        ring_copy(step, d, ch).wait_recv()
        pair_copy(band, ch, False).start()
        mine = low if step > 0 else high
        if d + 1 < half or (d + 1 == half and ch in mine):
            ring_copy(step, d, ch).start()

    def wait_pair(band, ch):
        pair_copy(band, ch, False).wait_recv()

    tile = max(t for t in range(128, 513, 128) if cells % t == 0)
    depth = 2 * rows

    depth2 = 2 * quarter

    def wait_chip(c):
        for ch in range(CHUNKS):
            wait_pair(2 * c + 1 - core, ch)

    def both(ref, c, q, at):
        return jnp.concatenate(
            [ref[pl.ds(pl.multiple_of((2 * c + k) * rows + q * quarter, quarter), quarter), at] for k in range(2)]
        )

    def add_quarter(c, q, first=False):
        z_t[:, :depth2] = both(z_all, c, q, slice(None)).T

        @pl.loop(0, cells // tile)
        def _(i):
            at = pl.ds(pl.multiple_of(i * tile, tile), tile)
            term = jnp.dot(z_t[:, :depth2], both(w_all, c, q, at), preferred_element_type=jnp.float32)
            if first:
                total[:, at] = term
            else:
                total[:, at] += term

    def add_unit(c, dz):
        if dz == 0:
            add_quarter(c, g)
            return

        @pl.when(g - dz >= 0)
        def _():
            add_quarter(c, g - dz)

        @pl.when(g + dz < ng)
        def _():
            add_quarter(c, g + dz)

    for ch in range(CHUNKS):
        remote(slot(me, ch), slot(me, ch), d_send.at[chip, ch], w_recv.at[me, ch], me, g).wait_recv()
        wait_pair(partner, ch)
    add_quarter(chip, g, True)

    steps = (ng - 1) * nb
    spread = len(events)
    done = {(0, 0)}
    for e, (d, a, b) in enumerate(events):
        lax.fori_loop(steps * e // spread, steps * (e + 1) // spread, z_step, 0)
        arrive(1, d, a)
        arrive(-1, d, b)
        for dd in range(half):
            if dd > (e + 1) // CHUNKS:
                continue
            for dz in range(ng):
                if (dd, dz) in done or nb * dz > steps * (e + 1) // spread:
                    continue
                done.add((dd, dz))
                for step in (1, -1) if dd else (1,):
                    c = chip_at(place - step * dd, chips)
                    if dd and not any((dd, x) in done for x in range(dz)):
                        wait_chip(c)
                    add_unit(c, dz)

    last = chip_at(place + half, chips)
    depth = 2 * rows
    last_rows = pl.ds(pl.multiple_of(last * depth, depth), depth)
    z_t[...] = z_all[last_rows, :].T
    occ_tile = jnp.concatenate([o_col[...]] * (tile // 128), axis=1)
    wait_chip(last)

    @pl.loop(0, cells // tile)
    def _(i):
        at = pl.ds(pl.multiple_of(i * tile, tile), tile)
        term = jnp.dot(z_t[...], w_all[last_rows, at], preferred_element_type=jnp.float32)
        rounded = (total[:, at] + term).astype(jnp.bfloat16)
        out_buf[:, at] = rounded
        values = rounded.astype(jnp.float32)
        d_all[me, :, at] = jnp.sum(occ_tile * values * values, axis=0, keepdims=True)
        pltpu.make_async_copy(out_buf.at[:, at], rotated.at[:, at], o_sem.at[i]).start()

    def q_copy(to):
        return remote(d_all.at[me], d_all.at[me], q_send.at[to], q_recv.at[me], to, g)

    for d in range(1, nb):
        q_copy(lax.rem(me + d, nb)).start()

    for d in range(1, ng):
        a_copy(lax.rem(g + d, ng)).wait_send()

    def b_sent(to, carry):
        @pl.when(to != me)
        def _():
            remote(
                a_buf.at[0, :, pl.ds(0, cols)], piece(me, g), b_send.at[to], b_recv.at[me], to, g
            ).wait_send()

        return carry

    lax.fori_loop(0, nb, b_sent, 0)

    def z_sent(t, carry):
        q, j = t // nb, lax.rem(t, nb)

        @pl.when((q <= g) & (g < ng - 1))
        def _():
            z_copy(1, q, j).wait_send()

        @pl.when((q >= g) & (g > 0))
        def _():
            z_copy(-1, q, j).wait_send()

        return carry

    lax.fori_loop(0, ng * nb, z_sent, 0)
    for step in (1, -1):
        mine = low if step > 0 else high
        for d in range(half):
            for ch in (range(CHUNKS) if d + 1 < half else mine):
                ring_copy(step, d, ch).wait_send()
    for c in range(chips):
        for ch in range(CHUNKS):
            remote(slot(2 * c + core, ch), slot(2 * c + core, ch), d_send.at[c, ch], w_recv.at[2 * c + core, ch], partner, g).wait_send()

    for d in range(1, nb):
        src = lax.rem(me + d, nb)
        remote(d_all.at[src], d_all.at[src], q_send.at[src], q_recv.at[src], me, g).wait_recv()
    density[...] = jnp.sum(d_all[...], axis=(0, 1)) / (nb * rows)
    for d in range(1, nb):
        q_copy(lax.rem(me + d, nb)).wait_send()

    @pl.loop(0, cells // tile)
    def _(i):
        at = pl.ds(pl.multiple_of(i * tile, tile), tile)
        pltpu.make_async_copy(out_buf.at[:, at], rotated.at[:, at], o_sem.at[i]).wait()


def solution(mesh):
    nb, ng = mesh.shape["band"], mesh.shape["grid"]

    def per_device(wave, ritz, occupation):
        rows, cells = wave.shape
        bands = rows * nb
        wide = ritz.shape[1]
        cols = bands // nb
        chips = nb // 2
        half = chips // 2
        dma = pltpu.SemaphoreType.DMA
        rotated, density = pl.pallas_call(
            functools.partial(kernel, nb, ng),
            out_shape=(
                jax.ShapeDtypeStruct((cols, cells), jnp.bfloat16),
                jax.ShapeDtypeStruct((cells,), jnp.float32),
            ),
            in_specs=[
                pl.BlockSpec(memory_space=pl.ANY),
                pl.BlockSpec(memory_space=pl.ANY),
                pl.BlockSpec(memory_space=pltpu.VMEM),
            ],
            out_specs=(pl.BlockSpec(memory_space=pl.ANY), pl.BlockSpec(memory_space=pltpu.VMEM)),
            scratch_shapes=[
                pltpu.VMEM((bands, cells), jnp.bfloat16),
                pltpu.VMEM((bands, cols), jnp.bfloat16),
                pltpu.VMEM((ng, rows // ng, wide), jnp.bfloat16),
                pltpu.VMEM((cols, 2 * rows), jnp.bfloat16),
                pltpu.VMEM((cols, cells), jnp.float32),
                pltpu.VMEM((cols, cells), jnp.bfloat16),
                pltpu.VMEM((nb, 1, cells), jnp.float32),
                pltpu.VMEM((cols, 128), jnp.float32),
                dma((ng,)), dma((ng,)), dma((nb,)), dma((nb,)),
                dma((ng, nb)), dma((ng, nb)), dma((ng, nb)),
                dma((half, CHUNKS)), dma((half, CHUNKS)), dma((chips, CHUNKS)), dma((nb, CHUNKS)),
                dma((nb,)), dma((nb,)), dma((cells // 128,)),
            ],
            compiler_params=pltpu.CompilerParams(
                collective_id=0, has_side_effects=True, vmem_limit_bytes=60 * 1024 * 1024
            ),
        )(wave, ritz, occupation[None, :])
        return rotated, density

    return jax.shard_map(
        per_device,
        mesh=mesh,
        in_specs=(P("band", "grid"), P("band", "grid"), P("band")),
        out_specs=(P("band", "grid"), P("grid")),
        check_vma=False,
    )
```

```python
import functools

import jax
import jax.numpy as jnp
from jax import lax
from jax.experimental import pallas as pl
from jax.experimental.pallas import tpu as pltpu
from jax.sharding import PartitionSpec as P

MESH = pl.DeviceIdType.MESH
CHUNKS = 8
AHEAD = 3
Z_AHEAD = 5


def chip_at(p, chips):
    p = lax.rem(p + chips, chips)
    back = (2 * p) // chips
    return (1 - back) * (2 * p) + back * (2 * (chips - 1 - p) + 1)


def kernel(
    nb, ng, wave, ritz, occ, rotated, density,
    w_all, z_all, a_buf, z_t, total, out_buf, d_all, o_col,
    a_send, a_recv, b_send, b_recv, up_send, dn_send, z_recv,
    r_send, l_send, d_send, w_recv, q_send, q_recv, o_sem,
):
    chips = nb // 2
    half = chips // 2
    rows, cells = wave.shape
    cols = z_all.shape[1]
    quarter = rows // ng
    crows = rows // CHUNKS
    me = lax.axis_index("band")
    g = lax.axis_index("grid")
    core = lax.rem(me, 2)
    chip = me // 2
    odd = lax.rem(chip, 2)
    place = (1 - odd) * (chip // 2) + odd * (chips - 1 - chip // 2)
    partner = me + 1 - 2 * core

    barrier = pltpu.get_barrier_semaphore()
    for d in range(1, nb):
        pl.semaphore_signal(barrier, inc=1, device_id={"band": lax.rem(me + d, nb), "grid": g}, device_id_type=MESH)
    for d in range(1, ng):
        pl.semaphore_signal(barrier, inc=1, device_id={"band": me, "grid": lax.rem(g + d, ng)}, device_id_type=MESH)
    pl.semaphore_wait(barrier, nb - 1 + ng - 1)

    def remote(src, dst, send, recv, band, grid):
        return pltpu.make_async_remote_copy(
            src_ref=src, dst_ref=dst, send_sem=send, recv_sem=recv,
            device_id={"band": band, "grid": grid}, device_id_type=MESH,
        )

    def a_copy(to):
        return remote(
            ritz.at[pl.ds(pl.multiple_of(to * quarter, quarter), quarter), :],
            a_buf.at[g], a_send.at[to], a_recv.at[g], me, to,
        )

    for d in range(1, ng):
        a_copy(lax.rem(g + d, ng)).start()
    a_own = pltpu.make_async_copy(
        ritz.at[pl.ds(pl.multiple_of(g * quarter, quarter), quarter), :], a_buf.at[g], a_recv.at[g]
    )
    a_own.start()

    def slot(band, ch):
        return w_all.at[pl.ds(pl.multiple_of(band * rows + ch * crows, crows), crows), :]

    def own_chunk(ch):
        return wave.at[pl.ds(ch * crows, crows), :]

    def ring_copy(step, d, ch):
        band = chip_at(place - step * d, chips) * 2 + core
        to = chip_at(place + step, chips) * 2 + core
        sems = r_send if step > 0 else l_send
        src = own_chunk(ch) if d == 0 else slot(band, ch)
        return remote(src, slot(band, ch), sems.at[d, ch], w_recv.at[band, ch], to, g)

    def pair_copy(band, ch, first):
        src = own_chunk(ch) if first else slot(band, ch)
        return remote(src, slot(band, ch), d_send.at[band // 2, ch], w_recv.at[band, ch], partner, g)

    low = list(range(CHUNKS // 2))
    high = list(range(CHUNKS // 2, CHUNKS))
    waiting = []
    for d in range(half):
        waiting += [(d, a, b) for a, b in zip(low + high, high + low)]
    waiting = waiting[: (half - 1) * CHUNKS + CHUNKS // 2]
    events = [(d + 1, a, b) for d, a, b in waiting]
    sent = [0]

    def send_until(count):
        while sent[0] < min(count, len(waiting)):
            d, a, b = waiting[sent[0]]
            ring_copy(1, d, a).start()
            ring_copy(-1, d, b).start()
            sent[0] += 1

    send_until(1)
    for ch in range(CHUNKS):
        pltpu.make_async_copy(own_chunk(ch), slot(me, ch), w_recv.at[me, ch]).start()
        pair_copy(me, ch, True).start()

    def piece(band, q):
        return z_all.at[pl.ds(pl.multiple_of(band * rows + q * quarter, quarter), quarter), :]

    def b_copy(c, k):
        return remote(
            a_buf.at[c, :, pl.ds(k * cols, cols)], piece(me, g),
            b_send.at[2 * c + k], b_recv.at[me], 2 * c + k, g,
        )

    def b_local(c, k):
        return pltpu.make_async_copy(a_buf.at[c, :, pl.ds(k * cols, cols)], piece(me, g), b_recv.at[me])

    for d in range(ng):
        c = lax.rem(g + d, ng)
        remote(a_buf.at[c], a_buf.at[c], a_send.at[c], a_recv.at[c], me, g).wait_recv()
        for k in range(2):
            @pl.when(2 * c + k == me)
            def _():
                b_local(c, k).start()

            @pl.when(2 * c + k != me)
            def _():
                b_copy(c, k).start()

        if d == 0:
            send_until(AHEAD)
    o_col[...] = jnp.broadcast_to(occ[...], (128, cols)).T

    def z_copy(step, q, j):
        sems = up_send if step > 0 else dn_send
        return remote(piece(j, q), piece(j, q), sems.at[q, j], z_recv.at[q, j], me, g + step)

    steps = (ng - 1) * nb

    def z_send(n):
        d = n // nb
        j = lax.rem(me + n, nb)

        @pl.when(d == 0)
        def _():
            remote(piece(j, g), piece(j, g), b_send.at[j], b_recv.at[j], me, g).wait_recv()

        @pl.when((g - d >= 0) & (g < ng - 1))
        def _():
            z_copy(1, g - d, j).start()

        @pl.when((g + d < ng) & (g > 0))
        def _():
            z_copy(-1, g + d, j).start()

    def z_first(n, carry):
        z_send(n)
        return carry

    lax.fori_loop(0, Z_AHEAD, z_first, 0)

    def z_step(t, carry):
        d = t // nb + 1
        j = lax.rem(me + t, nb)

        @pl.when(g - d >= 0)
        def _():
            z_copy(1, g - d, j).wait_recv()

        @pl.when(g + d < ng)
        def _():
            z_copy(-1, g + d, j).wait_recv()

        @pl.when(t + Z_AHEAD < steps)
        def _():
            z_send(t + Z_AHEAD)

        return carry

    def arrive(step, d, ch):
        band = chip_at(place - step * d, chips) * 2 + core
        ring_copy(step, d, ch).wait_recv()
        pair_copy(band, ch, False).start()

    def wait_pair(band, ch):
        pair_copy(band, ch, False).wait_recv()

    tile = max(t for t in range(128, 513, 128) if cells % t == 0)
    depth = 2 * rows

    depth2 = 2 * quarter

    def wait_chip(c):
        for ch in range(CHUNKS):
            wait_pair(2 * c + 1 - core, ch)

    def both(ref, c, q, at):
        return jnp.concatenate(
            [ref[pl.ds(pl.multiple_of((2 * c + k) * rows + q * quarter, quarter), quarter), at] for k in range(2)]
        )

    def add_quarter(c, q, first=False):
        z_t[:, :depth2] = both(z_all, c, q, slice(None)).T

        @pl.loop(0, cells // tile)
        def _(i):
            at = pl.ds(pl.multiple_of(i * tile, tile), tile)
            term = jnp.dot(z_t[:, :depth2], both(w_all, c, q, at), preferred_element_type=jnp.float32)
            if first:
                total[:, at] = term
            else:
                total[:, at] += term

    def add_unit(c, dz, first):
        if dz == 0:
            add_quarter(c, g, first)
            return

        @pl.when(g - dz >= 0)
        def _():
            add_quarter(c, g - dz)

        @pl.when(g + dz < ng)
        def _():
            add_quarter(c, g + dz)

    for ch in range(CHUNKS):
        remote(slot(me, ch), slot(me, ch), d_send.at[chip, ch], w_recv.at[me, ch], me, g).wait_recv()
        wait_pair(partner, ch)

    spread = len(events)
    done = set()
    for e, (d, a, b) in enumerate(events):
        lax.fori_loop(steps * e // spread, steps * (e + 1) // spread, z_step, 0)
        arrive(1, d, a)
        arrive(-1, d, b)
        send_until(e + 1 + AHEAD)
        for dd in range(half):
            if dd > (e + 1) // CHUNKS:
                continue
            for dz in range(ng):
                if (dd, dz) in done or max(nb * dz, nb - Z_AHEAD) > steps * (e + 1) // spread:
                    continue
                done.add((dd, dz))
                for step in (1, -1) if dd else (1,):
                    c = chip_at(place - step * dd, chips)
                    if dd and not any((dd, x) in done for x in range(dz)):
                        wait_chip(c)
                    add_unit(c, dz, dd == 0)

    last = chip_at(place + half, chips)
    depth = 2 * rows
    last_rows = pl.ds(pl.multiple_of(last * depth, depth), depth)
    z_t[...] = z_all[last_rows, :].T
    occ_tile = jnp.concatenate([o_col[...]] * (tile // 128), axis=1)
    wait_chip(last)

    @pl.loop(0, cells // tile)
    def _(i):
        at = pl.ds(pl.multiple_of(i * tile, tile), tile)
        term = jnp.dot(z_t[...], w_all[last_rows, at], preferred_element_type=jnp.float32)
        rounded = (total[:, at] + term).astype(jnp.bfloat16)
        out_buf[:, at] = rounded
        values = rounded.astype(jnp.float32)
        d_all[me, :, at] = jnp.sum(occ_tile * values * values, axis=0, keepdims=True)
        pltpu.make_async_copy(out_buf.at[:, at], rotated.at[:, at], o_sem.at[i]).start()

    def q_copy(to):
        return remote(d_all.at[me], d_all.at[me], q_send.at[to], q_recv.at[me], to, g)

    for d in range(1, nb):
        q_copy(lax.rem(me + d, nb)).start()

    for d in range(1, ng):
        a_copy(lax.rem(g + d, ng)).wait_send()

    def b_sent(to, carry):
        @pl.when(to != me)
        def _():
            remote(
                a_buf.at[0, :, pl.ds(0, cols)], piece(me, g), b_send.at[to], b_recv.at[me], to, g
            ).wait_send()

        return carry

    lax.fori_loop(0, nb, b_sent, 0)

    def z_sent(t, carry):
        q, j = t // nb, lax.rem(t, nb)

        @pl.when((q <= g) & (g < ng - 1))
        def _():
            z_copy(1, q, j).wait_send()

        @pl.when((q >= g) & (g > 0))
        def _():
            z_copy(-1, q, j).wait_send()

        return carry

    lax.fori_loop(0, ng * nb, z_sent, 0)
    for step in (1, -1):
        mine = low if step > 0 else high
        for d in range(half):
            for ch in (range(CHUNKS) if d + 1 < half else mine):
                ring_copy(step, d, ch).wait_send()
    for c in range(chips):
        for ch in range(CHUNKS):
            remote(slot(2 * c + core, ch), slot(2 * c + core, ch), d_send.at[c, ch], w_recv.at[2 * c + core, ch], partner, g).wait_send()

    for d in range(1, nb):
        src = lax.rem(me + d, nb)
        remote(d_all.at[src], d_all.at[src], q_send.at[src], q_recv.at[src], me, g).wait_recv()
    density[...] = jnp.sum(d_all[...], axis=(0, 1)) / (nb * rows)
    for d in range(1, nb):
        q_copy(lax.rem(me + d, nb)).wait_send()

    @pl.loop(0, cells // tile)
    def _(i):
        at = pl.ds(pl.multiple_of(i * tile, tile), tile)
        pltpu.make_async_copy(out_buf.at[:, at], rotated.at[:, at], o_sem.at[i]).wait()


def solution(mesh):
    nb, ng = mesh.shape["band"], mesh.shape["grid"]

    def per_device(wave, ritz, occupation):
        rows, cells = wave.shape
        bands = rows * nb
        wide = ritz.shape[1]
        cols = bands // nb
        chips = nb // 2
        half = chips // 2
        dma = pltpu.SemaphoreType.DMA
        rotated, density = pl.pallas_call(
            functools.partial(kernel, nb, ng),
            out_shape=(
                jax.ShapeDtypeStruct((cols, cells), jnp.bfloat16),
                jax.ShapeDtypeStruct((cells,), jnp.float32),
            ),
            in_specs=[
                pl.BlockSpec(memory_space=pl.ANY),
                pl.BlockSpec(memory_space=pl.ANY),
                pl.BlockSpec(memory_space=pltpu.VMEM),
            ],
            out_specs=(pl.BlockSpec(memory_space=pl.ANY), pl.BlockSpec(memory_space=pltpu.VMEM)),
            scratch_shapes=[
                pltpu.VMEM((bands, cells), jnp.bfloat16),
                pltpu.VMEM((bands, cols), jnp.bfloat16),
                pltpu.VMEM((ng, rows // ng, wide), jnp.bfloat16),
                pltpu.VMEM((cols, 2 * rows), jnp.bfloat16),
                pltpu.VMEM((cols, cells), jnp.float32),
                pltpu.VMEM((cols, cells), jnp.bfloat16),
                pltpu.VMEM((nb, 1, cells), jnp.float32),
                pltpu.VMEM((cols, 128), jnp.float32),
                dma((ng,)), dma((ng,)), dma((nb,)), dma((nb,)),
                dma((ng, nb)), dma((ng, nb)), dma((ng, nb)),
                dma((half, CHUNKS)), dma((half, CHUNKS)), dma((chips, CHUNKS)), dma((nb, CHUNKS)),
                dma((nb,)), dma((nb,)), dma((cells // 128,)),
            ],
            compiler_params=pltpu.CompilerParams(
                collective_id=0, has_side_effects=True, vmem_limit_bytes=60 * 1024 * 1024
            ),
        )(wave, ritz, occupation[None, :])
        return rotated, density

    return jax.shard_map(
        per_device,
        mesh=mesh,
        in_specs=(P("band", "grid"), P("band", "grid"), P("band")),
        out_specs=(P("band", "grid"), P("grid")),
        check_vma=False,
    )
```
